32 devices in a mesh: unit: 4 (over y, core), zero: 4 (over z), cols: 2 (over x).
Axes of the slice: x: 2, y: 2, z: 4, core: 2. Of those that a mesh axis runs over, the one named last changes fastest.
Arguments:
- weight_gate: bfloat16 [20480, 13824], P(('unit', 'zero'), 'cols'), parts along dimension 0, may hold values from -0.125 to 0.125
- low_gate: bfloat16 [20480, 32], P(('unit', 'zero')), parts along dimension 0, may hold values from -0.078125 to 0.078125
- high_gate: bfloat16 [128, 13824], P('unit', 'cols'), parts along dimension 0, may hold values from -1 to 1
- weight_up: bfloat16 [20480, 13824], P(('unit', 'zero'), 'cols'), parts along dimension 0, may hold values from -0.125 to 0.125
- low_up: bfloat16 [20480, 32], P(('unit', 'zero')), parts along dimension 0, may hold values from -0.078125 to 0.078125
- high_up: bfloat16 [128, 13824], P('unit', 'cols'), parts along dimension 0, may hold values from -1 to 1
- norm_train: float32 [20480], P(('unit', 'zero', 'cols')), parts along dimension 0, may hold values from 0.25 to 1.75
- norm_step: float32 [20480], P(('unit', 'zero', 'cols')), parts along dimension 0, may hold values from -0.3 to 0.3
Outputs:
- final_gate: bfloat16 [20480, 13824], P('unit', ('cols', 'zero')), parts along dimension 0
- final_up: bfloat16 [20480, 13824], P('unit', ('cols', 'zero')), parts along dimension 0
- scale_gate: float32 [55296], P(('unit', 'cols', 'zero')), parts along dimension 0
- scale_up: float32 [55296], P(('unit', 'cols', 'zero')), parts along dimension 0
- serve_norm: bfloat16 [20480], P('unit'), parts along dimension 0
The draws below stay inside these ranges and needn't reach their ends.
There are 4 independent parts, one for each index of `unit`. The reference program is written for one: setup_inputs(seed, part) draws one part's arguments, and reference() takes and returns one part's arrays. A program takes and returns all parts, laid end to end along the dimension named above; each array names one. Nothing has to cross between parts.
All inputs are finite; a program needn't handle non-finite values. Where the reference program divides by a largest or mean magnitude, that divisor is 1e-20 or more.
Results may differ from the reference program's by a relative error of at most 0.001.
Values may be sent and summed in bfloat16 or wider, within the bound.
A program may use at most 192 MiB of HBM per device.

```python
import jax
import jax.numpy as jnp

D_MODEL = 5120
D_INNER = 13824
RANK = 32


def strengthened(entries, own_key, source, target, parts, factor):
    def block_of(position):
        return (jnp.arange(entries.shape[position]) // (entries.shape[position] // parts)).reshape((-1,) + (1,) * (entries.ndim - 1 - position))

    one_side = jax.random.permutation(own_key, parts)[block_of(target)]
    other_side = (block_of(target) + parts // 2) % parts
    return jnp.where((block_of(source) == one_side) | (block_of(source) == other_side), factor * entries, entries)


def levels(own_key, extent, split, least, top_value):
    level, own = 1.0, jax.random.fold_in(own_key, 6)
    for dim, blocks in split:
        draws = jnp.exp(jax.random.uniform(jax.random.fold_in(own, dim), (blocks,), jnp.float32, least / len(split), top_value / len(split)))
        level = level * jnp.repeat(draws, extent[dim] // blocks).reshape([-1 if axis == dim else 1 for axis in range(len(extent))])
    return level


def normal_values(rng, extent, deviation, most, cuts=(), kind=jnp.bfloat16):
    level = levels(rng, extent, cuts, -0.22, 0.18) if cuts else 1.0
    entries = jax.random.normal(rng, extent, jnp.float32) * deviation * level
    return jnp.minimum(jnp.maximum(entries, -most), most).astype(kind)


def gaussian_with(stream_key, extent, width, bound, shards, heavy, held_as=jnp.bfloat16):
    values = width * jax.random.normal(stream_key, extent, jnp.float32)
    if shards:
        values = values * levels(stream_key, extent, shards, -0.22, 0.18)
    return jnp.clip(strengthened(values, jax.random.fold_in(stream_key, 3), *heavy), -bound, bound).astype(held_as)


def setup_inputs(seed: int = 0, part: int = 0) -> dict:
    keys = jax.random.split(jax.random.key(seed), 9)
    part_splits = jax.random.split(jax.random.fold_in(keys[8], part), 9)
    return {
        "weight_gate": gaussian_with(part_splits[0], (D_MODEL, D_INNER), D_MODEL ** -0.5, 0.125, ((0, 4), (1, 2)), (0, 1, 4, 2.0)),
        "low_gate": normal_values(part_splits[1], (D_MODEL, RANK), D_MODEL ** -0.5, 0.078125, ((0, 4),)),
        "high_gate": normal_values(part_splits[2], (RANK, D_INNER), RANK ** -0.5, 1.0, ((1, 2),)),
        "weight_up": gaussian_with(part_splits[3], (D_MODEL, D_INNER), D_MODEL ** -0.5, 0.125, ((0, 4), (1, 2)), (0, 1, 4, 2.0)),
        "low_up": normal_values(part_splits[4], (D_MODEL, RANK), D_MODEL ** -0.5, 0.078125, ((0, 4),)),
        "high_up": normal_values(part_splits[5], (RANK, D_INNER), RANK ** -0.5, 1.0, ((1, 2),)),
        "norm_train": jnp.clip(1.0 + 0.15 * jax.random.normal(part_splits[6], (D_MODEL,), jnp.float32), 0.25, 1.75),
        "norm_step": jnp.clip(jax.random.uniform(part_splits[7], (D_MODEL,), jnp.float32, -0.3, 0.3) * levels(part_splits[7], (D_MODEL,), ((0, 8),), -0.4, 0.0), -0.3, 0.3),
    }


mix_rate = 0.5


def reference(weight_gate, low_gate, high_gate, weight_up, low_up, high_up, norm_train, norm_step):
    result_gate = weight_gate.astype(jnp.float32) + mix_rate * jnp.dot(low_gate, high_gate, preferred_element_type=jnp.float32)
    result_up = weight_up.astype(jnp.float32) + mix_rate * jnp.dot(low_up, high_up, preferred_element_type=jnp.float32)
    scale_gate = jnp.sum(jnp.abs(result_gate), axis=0) / D_MODEL
    final_gate = (result_gate / scale_gate).astype(jnp.bfloat16)
    scale_up = jnp.sum(jnp.abs(result_up), axis=0) / D_MODEL
    final_up = (result_up / scale_up).astype(jnp.bfloat16)
    serve_norm = (norm_train + norm_step).astype(jnp.bfloat16)
    return final_gate, final_up, scale_gate, scale_up, serve_norm
```

```python
import jax
import jax.numpy as jnp
from jax import lax
from jax.experimental import pallas as pl
from jax.experimental.pallas import tpu as pltpu
from jax.sharding import PartitionSpec as P

mix_rate = 0.5


def cuts(units, shares):
    total, marks, seen = sum(shares), [0], 0
    for share in shares:
        seen += share
        marks.append(units * seen // total)
    return [(a, b) for a, b in zip(marks[:-1], marks[1:]) if b > a]


def merge_kernel(block_ref, low_ref, high_ref, *refs):
    final_ref, scale_ref, result_ref = refs[-3:]
    n, _, rows = block_ref.shape
    change = mix_rate * jnp.dot(high_ref[...], low_ref[...], preferred_element_type=jnp.float32)
    total = None
    for s in range(n):
        part = block_ref[s].astype(jnp.float32) + change[:, s * rows : (s + 1) * rows]
        result_ref[:, s * rows : (s + 1) * rows] = part
        size = jnp.sum(jnp.abs(part), axis=1, keepdims=True)
        total = size if total is None else total + size
    scale = total / (n * rows)
    scale_ref[...] = scale
    final_ref[...] = (result_ref[...] / scale).astype(final_ref.dtype)


def merge(block, low, high, final, first, step, width):
    n, part, rows = block.shape
    rank = low.shape[0]
    offset = first // step
    operands = [block, low, high]
    in_specs = [
        pl.BlockSpec((n, step, rows), lambda i: (0, i, 0)),
        pl.BlockSpec((rank, n * rows), lambda i: (0, 0)),
        pl.BlockSpec((step, rank), lambda i: (i + offset, 0)),
    ]
    aliases = {}
    if final is not None:
        operands.append(final)
        in_specs.append(pl.BlockSpec(memory_space=pl.ANY))
        aliases = {3: 0}
    return pl.pallas_call(
        merge_kernel,
        grid=(part // step,),
        in_specs=in_specs,
        out_specs=[
            pl.BlockSpec((step, n * rows), lambda i: (i + offset, 0)),
            pl.BlockSpec((step, 1), lambda i: (i, 0)),
        ],
        out_shape=[
            jax.ShapeDtypeStruct((width, n * rows), jnp.bfloat16),
            jax.ShapeDtypeStruct((part, 1), jnp.float32),
        ],
        scratch_shapes=[pltpu.VMEM((step, n * rows), jnp.float32)],
        input_output_aliases=aliases,
        cost_estimate=pl.CostEstimate(
            flops=2 * part * n * rows * rank,
            bytes_accessed=4 * part * n * rows,
            transcendentals=0,
        ),
        compiler_params=pltpu.CompilerParams(vmem_limit_bytes=24 << 20),
    )(*operands)


def local(weight_gate, low_gate, high_gate, weight_up, low_up, high_up, norm_train, norm_step):
    n = lax.axis_size("zero")
    rows, width = weight_gate.shape[0], weight_gate.shape[1] // n
    rank = low_gate.shape[1]
    place = lax.axis_index("zero")
    step = next(s for s in (48, 24, 16, 8, width) if width % s == 0)

    lows = lax.all_gather(
        jnp.concatenate([low_gate.T, low_up.T], axis=0), "zero", axis=1, tiled=True
    )
    serve_norm = lax.all_gather(
        (norm_train + norm_step).astype(jnp.bfloat16), ("zero", "cols"), axis=0, tiled=True
    )
    lows, serve_norm, weight_gate, weight_up = lax.optimization_barrier(
        (lows, serve_norm, weight_gate, weight_up)
    )
    low = {"gate": lows[:rank], "up": lows[rank:]}
    high = {
        "gate": lax.dynamic_slice_in_dim(high_gate, place * width, width, axis=1).T,
        "up": lax.dynamic_slice_in_dim(high_up, place * width, width, axis=1).T,
    }
    turned = {
        "gate": weight_gate.T.reshape(n, width, rows),
        "up": weight_up.T.reshape(n, width, rows),
    }

    shares = {"gate": (1, 3), "up": (7, 2)}
    jobs = [
        (name, a * step, b * step)
        for name in ("gate", "up")
        for a, b in cuts(width // step, shares[name])
    ]
    finals = {"gate": None, "up": None}
    scales = {"gate": [], "up": []}
    block = None
    arrived = []
    for name, a, b in jobs:
        sent = turned[name][:, a:b]
        if block is not None:
            sent, block = lax.optimization_barrier((sent, block))
            arrived.append(block)
        block = lax.all_to_all(sent, "zero", split_axis=0, concat_axis=0, tiled=True)
    arrived.append(block)
    for (name, a, b), block in zip(jobs, arrived):
        finals[name], scale = merge(block, low[name], high[name], finals[name], a, step, width)
        scales[name].append(scale[:, 0])
    return (
        finals["gate"].T,
        finals["up"].T,
        jnp.concatenate(scales["gate"]),
        jnp.concatenate(scales["up"]),
        serve_norm,
    )


def solution(mesh):
    in_specs = (
        P(("unit", "zero"), "cols"),
        P(("unit", "zero"), None),
        P("unit", "cols"),
        P(("unit", "zero"), "cols"),
        P(("unit", "zero"), None),
        P("unit", "cols"),
        P(("unit", "zero", "cols")),
        P(("unit", "zero", "cols")),
    )
    out_specs = (
        P("unit", ("cols", "zero")),
        P("unit", ("cols", "zero")),
        P(("unit", "cols", "zero")),
        P(("unit", "cols", "zero")),
        P("unit"),
    )
    return jax.shard_map(local, mesh=mesh, in_specs=in_specs, out_specs=out_specs, check_vma=False)
```
